32 devices in a mesh: seq: 4 (over y, core), span: 8 (over z, x).
Axes of the slice: x: 2, y: 2, z: 4, core: 2. Of those that a mesh axis runs over, the one named last changes fastest.
Arguments:
- queries: bfloat16 [8, 512, 1536], P('span', 'seq'), may hold values from -6 to 6
- key_head_matrix: bfloat16 [8, 512, 512], P('span', 'seq'), may hold values from -6 to 6
- value_head_matrix: bfloat16 [8, 512, 512], P('span', 'seq'), may hold values from -6 to 6
- attn_output: bfloat16 [8, 512, 1536], P('span', 'seq'), may hold values from -6 to 6
- out_grad: bfloat16 [8, 512, 1536], P('span', 'seq'), may hold values from -6 to 6
Outputs:
- query_grad: bfloat16 [8, 512, 1536], P('span', 'seq')
- key_grad: bfloat16 [8, 512, 512], P('span', 'seq')
- value_grad: bfloat16 [8, 512, 512], P('span', 'seq')
The draws below stay inside these ranges and needn't reach their ends.
All inputs are finite; a program needn't handle non-finite values.
Results may differ from the reference program's by a relative error of at most 0.005.
Values may be sent and summed in bfloat16 or wider, within the bound.
A program may use at most 64 MiB of HBM per device.

```python
import math
import jax
import jax.numpy as jnp
from jax import lax

HEAD_WIDTH = 64
KEY_HEADS = 8
QUERY_PER_KEY = 3
HQ = 24
BLOCK_TOKENS = 512
SEQUENCE_BLOCKS = 8


def draw_queries(key, part):
    random_seed_key = jax.random.fold_in(key, 1)
    value_rows = jax.random.truncated_normal(random_seed_key, -6.0, 6.0, (SEQUENCE_BLOCKS, BLOCK_TOKENS, HQ * HEAD_WIDTH), jnp.float32)
    return value_rows.astype(jnp.bfloat16)


def draw_key_head_matrix(key, part):
    random_seed_key = jax.random.fold_in(key, 2)
    value_rows = jax.random.truncated_normal(random_seed_key, -6.0, 6.0, (SEQUENCE_BLOCKS, BLOCK_TOKENS, KEY_HEADS * HEAD_WIDTH), jnp.float32)
    return value_rows.astype(jnp.bfloat16)


def shard_levels(own_key, shape, split, smallest, largest):
    gain = 1.0
    for position, blocks in split:
        heights = jax.random.uniform(jax.random.fold_in(jax.random.fold_in(own_key, 6), position), (blocks,), jnp.float32, smallest / len(split), largest / len(split))
        gain = gain * jnp.repeat(jnp.exp(heights), shape[position] // blocks).reshape((-1,) + (1,) * (len(shape) - 1 - position))
    return gain


def bell_draw(own_key, extent, scale, limit, split=(), held_as=jnp.bfloat16):
    values = jax.random.normal(own_key, extent, jnp.float32) * scale
    if len(split) > 0:
        values = shard_levels(own_key, extent, split, -0.22, 0.18) * values
    return jnp.clip(values, min=-limit, max=limit).astype(held_as)


def setup_inputs(seed: int = 0) -> dict:
    key_of = jax.random.split(jax.random.key(seed), 6)
    queries = draw_queries(jax.random.fold_in(key_of[5], 71), 0)
    key_head_matrix = draw_key_head_matrix(jax.random.fold_in(key_of[5], 71), 0)
    value_head_matrix = bell_draw(key_of[2], (SEQUENCE_BLOCKS, BLOCK_TOKENS, KEY_HEADS * HEAD_WIDTH), 1.0, 6.0, ((0, 8), (1, 4)))
    attn_output = bell_draw(key_of[3], (SEQUENCE_BLOCKS, BLOCK_TOKENS, HQ * HEAD_WIDTH), 1.0, 6.0, ((0, 8), (1, 4)))
    out_grad = bell_draw(key_of[4], (SEQUENCE_BLOCKS, BLOCK_TOKENS, HQ * HEAD_WIDTH), 1.0, 6.0, ((0, 8), (1, 4)))
    return {"queries": queries, "key_head_matrix": key_head_matrix, "value_head_matrix": value_head_matrix, "attn_output": attn_output, "out_grad": out_grad}


NEG_LARGE = -1e+30

def head_grads(running, inputs):
    query_head, key_head, value_head, output_head, grad_head = inputs
    sequence_length = query_head.shape[0]
    scaling = 1.0 / math.sqrt(HEAD_WIDTH)
    positions = lax.iota(jnp.int32, sequence_length)
    allowed = positions[None, :] <= positions[:, None]
    scores = jnp.dot(query_head, key_head.T, preferred_element_type=jnp.float32) * scaling
    row_max = lax.optimization_barrier(jnp.max(jnp.where(allowed, scores, NEG_LARGE), axis=1))
    row_sum = lax.optimization_barrier(jnp.sum(jnp.where(allowed, jnp.exp(scores - row_max[:, None]), 0.0), axis=1))
    log_norm = row_max + jnp.log(row_sum)
    prob_weights = jnp.where(allowed, jnp.exp(scores - log_norm[:, None]), 0.0)
    row_delta = lax.optimization_barrier(jnp.sum(grad_head.astype(jnp.float32) * output_head.astype(jnp.float32), axis=1))
    prob_grad = jnp.dot(grad_head, value_head.T, preferred_element_type=jnp.float32)
    score_low = (prob_weights * (prob_grad - row_delta[:, None])).astype(jnp.bfloat16)
    prob_low = prob_weights.astype(jnp.bfloat16)
    query_part = scaling * jnp.dot(score_low, key_head, preferred_element_type=jnp.float32)
    key_piece = scaling * jnp.dot(score_low.T, query_head, preferred_element_type=jnp.float32)
    value_piece = jnp.dot(prob_low.T, grad_head, preferred_element_type=jnp.float32)
    return (running, (query_part, key_piece, value_piece))

def reference(queries, key_head_matrix, value_head_matrix, attn_output, out_grad):
    sequence_length = SEQUENCE_BLOCKS * BLOCK_TOKENS

    def each_head_share(source, head_count):
        return jnp.transpose(source.reshape(sequence_length, head_count, HEAD_WIDTH), (1, 0, 2))
    key_complete = jnp.repeat(each_head_share(key_head_matrix, KEY_HEADS), QUERY_PER_KEY, axis=0)
    value_complete = jnp.repeat(each_head_share(value_head_matrix, KEY_HEADS), QUERY_PER_KEY, axis=0)
    start_state = jnp.zeros((), jnp.float32)
    final_state, head_results = lax.scan(head_grads, start_state, (each_head_share(queries, HQ), key_complete, value_complete, each_head_share(attn_output, HQ), each_head_share(out_grad, HQ)))
    query_part, key_piece, value_piece = head_results
    query_out = jnp.transpose(query_part, (1, 0, 2)).reshape(SEQUENCE_BLOCKS, BLOCK_TOKENS, HQ * HEAD_WIDTH).astype(jnp.bfloat16)
    key_total = lax.optimization_barrier(jnp.sum(key_piece.reshape(KEY_HEADS, QUERY_PER_KEY, sequence_length, HEAD_WIDTH), axis=1))
    value_total = lax.optimization_barrier(jnp.sum(value_piece.reshape(KEY_HEADS, QUERY_PER_KEY, sequence_length, HEAD_WIDTH), axis=1))
    key_result = jnp.transpose(key_total, (1, 0, 2)).reshape(SEQUENCE_BLOCKS, BLOCK_TOKENS, KEY_HEADS * HEAD_WIDTH).astype(jnp.bfloat16)
    value_result = jnp.transpose(value_total, (1, 0, 2)).reshape(SEQUENCE_BLOCKS, BLOCK_TOKENS, KEY_HEADS * HEAD_WIDTH).astype(jnp.bfloat16)
    return (query_out, key_result, value_result)
```

```python
import functools
import math

import jax
import jax.numpy as jnp
from jax import lax
from jax.experimental import pallas as pl
from jax.experimental.pallas import tpu as pltpu
from jax.sharding import PartitionSpec as P

HEAD_WIDTH = 64
QUERY_PER_KEY = 3
NEG_LARGE = -1e30
MESH = pl.DeviceIdType.MESH
LOG2E = math.log2(math.e)
SCORE_BYTES = 26 * 2**20


def place(group):
    seq_count = lax.axis_size("seq")
    span = lax.axis_index("span")
    layers = lax.axis_size("span") // group
    mine = lax.rem(span, group) * seq_count + lax.axis_index("seq")
    return span // group, mine, layers, group * seq_count


def device_of(layer, spot, group):
    seq_count = lax.axis_size("seq")
    return {"seq": lax.rem(spot, seq_count), "span": layer * group + spot // seq_count}


def spread_kernel(group, qg_ref, kv_ref, dl_ref, qg_out, kv_out, dl_out,
                  send_sem, recv_sem, kv_send, kv_recv, local_sem):
    layer, mine, layers, spots = place(group)

    def kv_copy(step, offset):
        spot = lax.rem(mine + offset, spots)
        return pltpu.make_async_remote_copy(
            src_ref=kv_ref.at[spot], dst_ref=kv_out.at[layer, mine],
            send_sem=kv_send.at[step, offset], recv_sem=kv_recv.at[step, offset],
            device_id=device_of(lax.rem(layer + step, layers), spot, group), device_id_type=MESH)

    def side_copy(which, offset):
        source, target = ((qg_ref, qg_out), (dl_ref, dl_out))[which]
        spot = lax.rem(mine + offset, spots)
        return pltpu.make_async_remote_copy(
            src_ref=source.at[spot], dst_ref=target.at[mine],
            send_sem=send_sem.at[which, offset], recv_sem=recv_sem.at[which, offset],
            device_id=device_of(layer, spot, group), device_id_type=MESH)

    for step in range(layers - 1, 0, -1):
        @pl.when(layer + step < layers)
        def _():
            for offset in range(spots):
                kv_copy(step, offset).start()

    for offset in range(1, spots):
        side_copy(0, offset).start()
        side_copy(1, offset).start()
        kv_copy(0, offset).start()
    own = (
        pltpu.make_async_copy(qg_ref.at[mine], qg_out.at[mine], local_sem.at[0]),
        pltpu.make_async_copy(dl_ref.at[mine], dl_out.at[mine], local_sem.at[1]),
        pltpu.make_async_copy(kv_ref.at[mine], kv_out.at[layer, mine], local_sem.at[2]),
    )
    for copy in own:
        copy.start()
    for copy in own:
        copy.wait()
    for offset in range(1, spots):
        side_copy(0, offset).wait()
        side_copy(1, offset).wait()
        kv_copy(0, offset).wait()
    for step in range(1, layers):
        @pl.when(layer + step < layers)
        def _():
            for offset in range(spots):
                kv_copy(step, offset).wait_send()

        @pl.when(layer - step >= 0)
        def _():
            for offset in range(spots):
                kv_copy(step, offset).wait_recv()


def collect_kernel(group, dq_ref, dkv_ref, dq_out, dkv_out, send_sem, recv_sem, kv_send, kv_recv, local_sem):
    layer, mine, layers, spots = place(group)

    def kv_copy(step, offset):
        spot = lax.rem(mine + offset, spots)
        below = lax.rem(layer - step + layers, layers)
        return pltpu.make_async_remote_copy(
            src_ref=dkv_ref.at[below, spot], dst_ref=dkv_out.at[layer, mine],
            send_sem=kv_send.at[step, offset], recv_sem=kv_recv.at[step, offset],
            device_id=device_of(below, spot, group), device_id_type=MESH)

    def side_copy(offset):
        spot = lax.rem(mine + offset, spots)
        return pltpu.make_async_remote_copy(
            src_ref=dq_ref.at[spot], dst_ref=dq_out.at[mine],
            send_sem=send_sem.at[offset], recv_sem=recv_sem.at[offset],
            device_id=device_of(layer, spot, group), device_id_type=MESH)

    for step in range(layers - 1, 0, -1):
        @pl.when(layer - step >= 0)
        def _():
            for offset in range(spots):
                kv_copy(step, offset).start()

    for offset in range(1, spots):
        side_copy(offset).start()
        kv_copy(0, offset).start()
    own = (
        pltpu.make_async_copy(dq_ref.at[mine], dq_out.at[mine], local_sem.at[0]),
        pltpu.make_async_copy(dkv_ref.at[layer, mine], dkv_out.at[layer, mine], local_sem.at[1]),
    )
    for copy in own:
        copy.start()
    for copy in own:
        copy.wait()
    for offset in range(1, spots):
        side_copy(offset).wait()
        kv_copy(0, offset).wait()
    for step in range(1, layers):
        @pl.when(layer - step >= 0)
        def _():
            for offset in range(spots):
                kv_copy(step, offset).wait_send()

        @pl.when(layer + step < layers)
        def _():
            for offset in range(spots):
                kv_copy(step, offset).wait_recv()


def dot(a, b, contract):
    return lax.dot_general(a, b, ((contract[:1], contract[1:]), ((), ())), preferred_element_type=jnp.float32)


def grads_kernel(tq, tk, layer_ref, qg_ref, kv_ref, dl_ref, dq_ref, dkv_ref,
                 s_ref, q_pad, g_pad, m_ref, l_ref, dqt_ref, acc_ref):
    rows = qg_ref.shape[0]
    width = HEAD_WIDTH * QUERY_PER_KEY
    scaling = 1.0 / math.sqrt(HEAD_WIDTH)
    factor = scaling * LOG2E
    first = layer_ref[0] * rows
    total_blocks = (first + rows) // tk

    def clear(j, _):
        at = pl.ds(pl.multiple_of(j * tk, tk), tk)
        acc_ref[at, :] = jnp.zeros((tk, 2 * HEAD_WIDTH), jnp.float32)
        return 0

    lax.fori_loop(0, total_blocks, clear, 0)

    def tile(i, _):
        q_rows = pl.ds(pl.multiple_of(i * tq, tq), tq)
        zero = jnp.zeros((tq, HEAD_WIDTH), jnp.bfloat16)
        for h in range(QUERY_PER_KEY):
            low = h * HEAD_WIDTH
            q_pad[h] = jnp.concatenate([qg_ref[q_rows, low:low + HEAD_WIDTH], zero], axis=1)
            g_pad[h] = jnp.concatenate([zero, qg_ref[q_rows, width + low:width + low + HEAD_WIDTH]], axis=1)
        m_ref[...] = jnp.full(m_ref.shape, NEG_LARGE, jnp.float32)
        l_ref[...] = jnp.zeros(l_ref.shape, jnp.float32)
        dqt_ref[...] = jnp.zeros(dqt_ref.shape, jnp.float32)
        q_first = first + i * tq
        last = q_first // tk

        def stats(j, masked):
            at = pl.ds(pl.multiple_of(j * tk, tk), tk)
            kv = kv_ref[at, :]
            for h in range(QUERY_PER_KEY):
                s = dot(kv, q_pad[h], (1, 1))
                if masked:
                    k_pos = j * tk + lax.broadcasted_iota(jnp.int32, (tk, tq), 0)
                    q_pos = q_first + lax.broadcasted_iota(jnp.int32, (tk, tq), 1)
                    s = jnp.where(k_pos <= q_pos, s, NEG_LARGE)
                s_ref[h, at, :] = s
                m_old = m_ref[h]
                m_new = jnp.maximum(m_old, jnp.max(s, axis=0, keepdims=True))
                e = jnp.exp2((s - m_new) * factor)
                l_ref[h] = l_ref[h] * jnp.exp2((m_old - m_new) * factor) + jnp.sum(e, axis=0, keepdims=True)
                m_ref[h] = m_new
            return 0

        lax.fori_loop(0, last, lambda j, _: stats(j, False), 0)
        stats(last, True)
        for h in range(QUERY_PER_KEY):
            m_ref[h] = m_ref[h] * factor + jnp.log2(l_ref[h])

        def grads(j, _):
            at = pl.ds(pl.multiple_of(j * tk, tk), tk)
            kv = kv_ref[at, :]
            k_turned = kv[:, :HEAD_WIDTH].T
            term = acc_ref[at, :]
            for h in range(QUERY_PER_KEY):
                p = jnp.exp2(s_ref[h, at, :] * factor - m_ref[h])
                dp = dot(kv, g_pad[h], (1, 1))
                ds = (p * (dp - dl_ref[pl.ds(h, 1), q_rows])).astype(jnp.bfloat16)
                term += dot(ds, q_pad[h], (1, 0))
                term += dot(p.astype(jnp.bfloat16), g_pad[h], (1, 0))
                dqt_ref[h] += dot(k_turned, ds, (1, 0))
            acc_ref[at, :] = term
            return 0

        lax.fori_loop(0, last + 1, grads, 0)
        dq = jnp.concatenate([dqt_ref[h].T for h in range(QUERY_PER_KEY)], axis=1)
        dq_ref[q_rows, :] = (dq * scaling).astype(jnp.bfloat16)
        return 0

    lax.fori_loop(0, rows // tq, tile, 0)

    def finish(j, _):
        at = pl.ds(pl.multiple_of(j * tk, tk), tk)
        lane = lax.broadcasted_iota(jnp.int32, (1, 2 * HEAD_WIDTH), 1)
        dkv_ref[at, :] = (acc_ref[at, :] * jnp.where(lane < HEAD_WIDTH, scaling, 1.0)).astype(jnp.bfloat16)
        return 0

    lax.fori_loop(0, total_blocks, finish, 0)


def vmem(count):
    return [pl.BlockSpec(memory_space=pltpu.VMEM)] * count


def per_device(queries, key_head_matrix, value_head_matrix, attn_output, out_grad):
    seq_count = lax.axis_size("seq")
    tokens = queries.shape[1]
    group = key_head_matrix.shape[2] // (HEAD_WIDTH * seq_count)
    layers = lax.axis_size("span") // group
    spots = group * seq_count
    width = HEAD_WIDTH * QUERY_PER_KEY
    rows = spots * tokens
    params = pltpu.CompilerParams(has_side_effects=True, vmem_limit_bytes=60 * 2**20)

    def by_spot(source):
        split = source.reshape(tokens, seq_count, group, source.shape[-1] // spots)
        return jnp.transpose(split, (2, 1, 0, 3)).reshape(spots, tokens, -1)

    qg = jnp.concatenate([by_spot(queries[0]), by_spot(out_grad[0])], axis=2)
    kv = jnp.concatenate([by_spot(key_head_matrix[0]), by_spot(value_head_matrix[0])], axis=2)
    product = out_grad[0].astype(jnp.float32) * attn_output[0].astype(jnp.float32)
    delta = jnp.sum(product.reshape(tokens, seq_count, group, QUERY_PER_KEY, HEAD_WIDTH), axis=4)
    delta = jnp.transpose(delta, (2, 1, 3, 0)).reshape(spots, QUERY_PER_KEY, tokens)
    delta = jnp.pad(delta, ((0, 0), (0, 8 - QUERY_PER_KEY), (0, 0)))

    qg_all, kv_all, dl_all = pl.pallas_call(
        functools.partial(spread_kernel, group),
        out_shape=(
            jax.ShapeDtypeStruct(qg.shape, jnp.bfloat16),
            jax.ShapeDtypeStruct((layers,) + kv.shape, jnp.bfloat16),
            jax.ShapeDtypeStruct(delta.shape, jnp.float32),
        ),
        in_specs=vmem(3),
        out_specs=tuple(vmem(3)),
        scratch_shapes=[
            pltpu.SemaphoreType.DMA((2, spots)),
            pltpu.SemaphoreType.DMA((2, spots)),
            pltpu.SemaphoreType.DMA((layers, spots)),
            pltpu.SemaphoreType.DMA((layers, spots)),
            pltpu.SemaphoreType.DMA((3,)),
        ],
        compiler_params=params,
        name="spread",
    )(qg, kv, delta)

    block = math.gcd(rows, 512)
    tk = block
    tq = block
    while QUERY_PER_KEY * layers * rows * tq * 4 > SCORE_BYTES and tq % 256 == 0:
        tq //= 2
    layer = (lax.axis_index("span") // group).reshape(1).astype(jnp.int32)
    dl_rows = jnp.transpose(dl_all, (1, 0, 2)).reshape(8, rows)
    stat = pltpu.VMEM((QUERY_PER_KEY, 1, tq), jnp.float32)
    dq, dkv = pl.pallas_call(
        functools.partial(grads_kernel, tq, tk),
        out_shape=(
            jax.ShapeDtypeStruct((rows, width), jnp.bfloat16),
            jax.ShapeDtypeStruct((layers * rows, 2 * HEAD_WIDTH), jnp.bfloat16),
        ),
        in_specs=[pl.BlockSpec(memory_space=pltpu.SMEM)] + vmem(3),
        out_specs=tuple(vmem(2)),
        scratch_shapes=[
            pltpu.VMEM((QUERY_PER_KEY, layers * rows, tq), jnp.float32),
            pltpu.VMEM((QUERY_PER_KEY, tq, 2 * HEAD_WIDTH), jnp.bfloat16),
            pltpu.VMEM((QUERY_PER_KEY, tq, 2 * HEAD_WIDTH), jnp.bfloat16),
            stat,
            stat,
            pltpu.VMEM((QUERY_PER_KEY, HEAD_WIDTH, tq), jnp.float32),
            pltpu.VMEM((layers * rows, 2 * HEAD_WIDTH), jnp.float32),
        ],
        compiler_params=pltpu.CompilerParams(vmem_limit_bytes=60 * 2**20),
        name="grads",
    )(layer, qg_all.reshape(rows, 2 * width), kv_all.reshape(layers * rows, 2 * HEAD_WIDTH), dl_rows)

    dq_all, dkv_all = pl.pallas_call(
        functools.partial(collect_kernel, group),
        out_shape=(
            jax.ShapeDtypeStruct((spots, tokens, width), jnp.bfloat16),
            jax.ShapeDtypeStruct((layers, spots, tokens, 2 * HEAD_WIDTH), jnp.bfloat16),
        ),
        in_specs=vmem(2),
        out_specs=tuple(vmem(2)),
        scratch_shapes=[
            pltpu.SemaphoreType.DMA((spots,)),
            pltpu.SemaphoreType.DMA((spots,)),
            pltpu.SemaphoreType.DMA((layers, spots)),
            pltpu.SemaphoreType.DMA((layers, spots)),
            pltpu.SemaphoreType.DMA((2,)),
        ],
        compiler_params=params,
        name="collect",
    )(dq.reshape(spots, tokens, width), dkv.reshape(layers, spots, tokens, 2 * HEAD_WIDTH))

    def by_token(source):
        split = source.reshape(group, seq_count, tokens, source.shape[-1])
        return jnp.transpose(split, (2, 1, 0, 3)).reshape(1, tokens, -1)

    came = lax.broadcasted_iota(jnp.int32, (layers, 1, 1, 1), 0) >= layer[0]
    kv_sum = jnp.sum(jnp.where(came, dkv_all.astype(jnp.float32), 0.0), axis=0).astype(jnp.bfloat16)
    return by_token(dq_all), by_token(kv_sum[..., :HEAD_WIDTH]), by_token(kv_sum[..., HEAD_WIDTH:])


def solution(mesh):
    spec = P("span", "seq", None)
    return jax.shard_map(
        per_device, mesh=mesh, in_specs=(spec,) * 5, out_specs=(spec,) * 3, check_vma=False
    )
```

```python
import functools
import math

import jax
import jax.numpy as jnp
from jax import lax
from jax.experimental import pallas as pl
from jax.experimental.pallas import tpu as pltpu
from jax.sharding import PartitionSpec as P

HEAD_WIDTH = 64
QUERY_PER_KEY = 3
NEG_LARGE = -1e30
MESH = pl.DeviceIdType.MESH
LOG2E = math.log2(math.e)
SCORE_BYTES = 17 * 2**20


def place(group):
    seq_count = lax.axis_size("seq")
    span = lax.axis_index("span")
    layers = lax.axis_size("span") // group
    mine = lax.rem(span, group) * seq_count + lax.axis_index("seq")
    return span // group, mine, layers, group * seq_count


def device_of(layer, spot, group):
    seq_count = lax.axis_size("seq")
    return {"seq": lax.rem(spot, seq_count), "span": layer * group + spot // seq_count}


def given_heads(layer, layers):
    surplus = QUERY_PER_KEY * 2 * (2 * layer + 1 - layers)
    count = (jnp.maximum(surplus, 0) + layer + 1) // (2 * layer + 2)
    return jnp.where(surplus > 0, jnp.minimum(count, QUERY_PER_KEY), 0)


def top_layer(layer, layers):
    mirror = layers - 1 - layer
    return jnp.where(given_heads(mirror, layers) > 0, mirror, layer)


def dot(a, b, contract):
    return lax.dot_general(a, b, ((contract[:1], contract[1:]), ((), ())), preferred_element_type=jnp.float32)


def kernel(group, tq, tk, qg_ref, kv_ref, dl_ref, dq_out, dkv_out,
           qg_in, kv_in, dl_in, s_ref, dl_row, dqt_ref, acc_ref, dq_ref, dkv_ref,
           q_send, q_recv, kv_send, kv_recv, dl_send, dl_recv,
           dq_send, dq_recv, ex_send, dkv_send, dkv_recv, q_local, dq_local, local_sem):
    layer, mine, layers, spots = place(group)
    heads = QUERY_PER_KEY
    half = spots // 2
    tokens = qg_ref.shape[2]
    rows = spots * tokens
    mirror = layers - 1 - layer
    given = given_heads(layer, layers)
    taken = given_heads(mirror, layers)
    top = top_layer(layer, layers)
    scaling = 1.0 / math.sqrt(HEAD_WIDTH)
    factor = scaling * LOG2E

    def spot_at(offset):
        return lax.rem(mine + offset, spots)

    def spot_from(offset):
        return lax.rem(mine + spots - offset, spots)

    def remote(source, target, send, recv, to_layer, spot):
        return pltpu.make_async_remote_copy(
            src_ref=source, dst_ref=target, send_sem=send, recv_sem=recv,
            device_id=device_of(to_layer, spot, group), device_id_type=MESH)

    def is_given(spot, h):
        return jnp.logical_and(spot >= half, h >= heads - given)

    def q_copy(h, offset):
        away = is_given(mine, h)
        slot = jnp.where(away, heads + h + given, (mine // half) * heads + h)
        spot = spot_at(offset)
        return remote(qg_ref.at[spot, h], qg_in.at[slot, lax.rem(mine, half)],
                      q_send.at[h, offset], q_recv.at[jnp.where(away, 1, 0), h, offset],
                      jnp.where(away, mirror, layer), spot)

    def q_arrival(kind, h, offset):
        return remote(qg_ref.at[0, h], qg_in.at[0, 0], q_send.at[h, offset], q_recv.at[kind, h, offset], mirror, mine)

    def q_own(h):
        return pltpu.make_async_copy(
            qg_ref.at[mine, h], qg_in.at[(mine // half) * heads + h, lax.rem(mine, half)], q_local.at[h])

    def dl_copy(kind, offset):
        spot = spot_at(offset)
        return remote(dl_ref.at[spot], dl_in.at[kind, mine], dl_send.at[kind, offset], dl_recv.at[kind, offset],
                      layer if kind == 0 else mirror, spot)

    def kv_copy(to_layer, offset):
        spot = spot_at(offset)
        return remote(kv_ref.at[spot], kv_in.at[layer, mine], kv_send.at[to_layer, offset],
                      kv_recv.at[layer, offset], to_layer, spot)

    def kv_arrival(from_layer, offset):
        return remote(kv_ref.at[0], kv_in.at[0, 0], kv_send.at[0, offset], kv_recv.at[from_layer, offset],
                      layer, mine)

    def dq_copy(slot_base, h, offset):
        spot = spot_at(offset)
        return remote(dq_ref.at[(spot // half) * heads + h, lax.rem(spot, half)], dq_out.at[mine, h],
                      dq_send.at[h, offset], dq_recv.at[h, offset], layer, spot)

    def dq_own(h):
        return pltpu.make_async_copy(
            dq_ref.at[(mine // half) * heads + h, lax.rem(mine, half)], dq_out.at[mine, h], dq_local.at[h])

    def dq_extra(k, u):
        spot = half + u
        h = heads - taken + k
        return remote(dq_ref.at[2 * heads + k, u], dq_out.at[mine, h], ex_send.at[k, u],
                      dq_recv.at[h, lax.rem(spot + spots - mine, spots)], mirror, spot)

    def dkv_copy(to_layer, offset):
        spot = spot_at(offset)
        return remote(dkv_ref.at[to_layer, spot], dkv_out.at[layer, mine], dkv_send.at[to_layer, offset],
                      dkv_recv.at[layer, offset], to_layer, spot)

    def dkv_arrival(from_layer, offset):
        return remote(dkv_ref.at[0, 0], dkv_out.at[0, 0], dkv_send.at[0, offset],
                      dkv_recv.at[from_layer, offset], layer, mine)

    kv_own = pltpu.make_async_copy(kv_ref.at[mine], kv_in.at[layer, mine], local_sem.at[0])
    dl_own = pltpu.make_async_copy(dl_ref.at[mine], dl_in.at[0, mine], local_sem.at[1])
    dkv_own = pltpu.make_async_copy(dkv_ref.at[layer, mine], dkv_out.at[layer, mine], local_sem.at[2])
    gives_now = jnp.logical_and(mine >= half, given > 0)

    for step in range(1, layers):
        other = lax.rem(layer + step, layers)

        @pl.when(top_layer(other, layers) >= layer)
        def _():
            for offset in range(spots):
                kv_copy(other, offset).start()

    kv_own.start()
    dl_own.start()
    for offset in range(1, spots):
        dl_copy(0, offset).start()
        kv_copy(layer, offset).start()
    for h in range(heads):
        for offset in range(1, spots):
            q_copy(h, offset).start()

        @pl.when(is_given(mine, h))
        def _():
            q_copy(h, 0).start()

        @pl.when(jnp.logical_not(is_given(mine, h)))
        def _():
            q_own(h).start()

    @pl.when(gives_now)
    def _():
        for offset in range(spots):
            dl_copy(1, offset).start()

    blocks_here = rows // tk

    def clear(j, _):
        acc_ref[pl.ds(pl.multiple_of(j * tk, tk), tk), :] = jnp.zeros((tk, 2 * HEAD_WIDTH), jnp.float32)
        return 0

    lax.fori_loop(0, (top + 1) * blocks_here, clear, 0)

    kv_own.wait()
    dl_own.wait()
    for offset in range(1, spots):
        dl_copy(0, offset).wait_recv()
        kv_arrival(layer, offset).wait_recv()
    for h in range(heads):
        for offset in range(1, spots):
            @pl.when(jnp.logical_not(is_given(spot_from(offset), h)))
            def _():
                q_arrival(0, h, offset).wait_recv()

        @pl.when(jnp.logical_not(is_given(mine, h)))
        def _():
            q_own(h).wait()

    def wait_layers(low, high):
        for other in range(layers):
            @pl.when(jnp.logical_and(other >= low, other < high))
            def _():
                for offset in range(spots):
                    kv_arrival(other, offset).wait_recv()

    wait_layers(0, layer)

    subs = half * tokens // tq
    pieces = tq // tokens
    lane = lax.broadcasted_iota(jnp.int32, (1, 2 * HEAD_WIDTH), 1)
    jobs = 2 * heads - given + taken

    def job(i, _):
        slot = i // subs
        sub = lax.rem(i, subs)
        extra = slot >= 2 * heads

        @pl.when(jnp.logical_and(extra, i == 2 * heads * subs))
        def _():
            for offset in range(spots):
                @pl.when(spot_from(offset) >= half)
                def _():
                    dl_copy(1, offset).wait_recv()
                    for h in range(heads):
                        @pl.when(h >= heads - taken)
                        def _():
                            q_arrival(1, h, offset).wait_recv()
            wait_layers(layer + 1, top + 1)

        q_layer = jnp.where(extra, mirror, layer)
        upper = slot >= heads
        head = jnp.where(extra, slot - heads - taken, lax.rem(slot, heads))
        q_first = q_layer * rows + jnp.where(upper, half * tokens, 0) + sub * tq
        last = q_first // tk
        both = qg_in[slot, pl.ds(sub * pieces, pieces)].reshape(tq, 2 * HEAD_WIDTH)
        q_pad = jnp.where(lane < HEAD_WIDTH, both, jnp.zeros_like(both))
        g_pad = jnp.where(lane < HEAD_WIDTH, jnp.zeros_like(both), both)
        for piece in range(pieces):
            spot = jnp.where(upper, half, 0) + sub * pieces + piece
            dl_row[:, piece * tokens:(piece + 1) * tokens] = dl_in[jnp.where(extra, 1, 0), spot, pl.ds(head, 1), :]
        dqt_ref[...] = jnp.zeros(dqt_ref.shape, jnp.float32)

        def kv_block(j):
            per = tk // tokens
            at = kv_in[j // blocks_here, pl.ds(lax.rem(j, blocks_here) * per, per)]
            return at.reshape(tk, 2 * HEAD_WIDTH)

        def stats(j, state, masked):
            m_old, total = state
            s = dot(kv_block(j), q_pad, (1, 1))
            if masked:
                k_pos = j * tk + lax.broadcasted_iota(jnp.int32, (tk, tq), 0)
                q_pos = q_first + lax.broadcasted_iota(jnp.int32, (tk, tq), 1)
                s = jnp.where(k_pos <= q_pos, s, NEG_LARGE)
            s_ref[pl.ds(pl.multiple_of(j * tk, tk), tk), :] = s
            m_new = jnp.maximum(m_old, jnp.max(s, axis=0, keepdims=True))
            e = jnp.exp2((s - m_new) * factor)
            return m_new, total * jnp.exp2((m_old - m_new) * factor) + jnp.sum(e, axis=0, keepdims=True)

        state = (jnp.full((1, tq), NEG_LARGE, jnp.float32), jnp.zeros((1, tq), jnp.float32))
        state = lax.fori_loop(0, last, lambda j, st: stats(j, st, False), state)
        m, total = stats(last, state, True)
        norm = m * factor + jnp.log2(total)
        delta = dl_row[...]

        def grads(j, _):
            at = pl.ds(pl.multiple_of(j * tk, tk), tk)
            kv = kv_block(j)
            p = jnp.exp2(s_ref[at, :] * factor - norm)
            dp = dot(kv, g_pad, (1, 1))
            ds = (p * (dp - delta)).astype(jnp.bfloat16)
            acc_ref[at, :] += dot(ds, q_pad, (1, 0)) + dot(p.astype(jnp.bfloat16), g_pad, (1, 0))
            dqt_ref[...] += dot(kv[:, :HEAD_WIDTH].T, ds, (1, 0))
            return 0

        def by_layer(l, _):
            lax.fori_loop(l * blocks_here, jnp.minimum((l + 1) * blocks_here, last + 1), grads, 0)

            @pl.when(i == jobs * subs - 1)
            def _():
                def finish(t, _):
                    at = pl.ds(pl.multiple_of(l * rows + t * tokens, tokens), tokens)
                    part = acc_ref[at, :] * jnp.where(lane < HEAD_WIDTH, scaling, 1.0)
                    dkv_ref[l, t] = part.astype(jnp.bfloat16)
                    return 0

                lax.fori_loop(0, spots, finish, 0)
                for offset in range(1, spots):
                    dkv_copy(l, offset).start()

                @pl.when(l == layer)
                def _():
                    dkv_own.start()

                @pl.when(l != layer)
                def _():
                    dkv_copy(l, 0).start()
            return 0

        lax.fori_loop(0, q_layer + 1, by_layer, 0)
        for piece in range(pieces):
            part = dqt_ref[:, piece * tokens:(piece + 1) * tokens] * scaling
            dq_ref[slot, sub * pieces + piece] = part.astype(jnp.bfloat16)

        @pl.when(sub == subs - 1)
        def _():
            @pl.when(extra)
            def _():
                for u in range(half):
                    dq_extra(slot - 2 * heads, u).start()

            @pl.when(jnp.logical_not(extra))
            def _():
                for offset in range(spots):
                    @pl.when(spot_at(offset) // half == slot // heads)
                    def _():
                        if offset:
                            dq_copy(0, head, offset).start()
                        else:
                            dq_own(head).start()
        return 0

    lax.fori_loop(0, jobs * subs, job, 0)

    for h in range(heads):
        for offset in range(1, spots):
            q_copy(h, offset).wait_send()

            @pl.when(jnp.logical_not(is_given(spot_at(offset), h)))
            def _():
                dq_copy(0, h, offset).wait_send()
            dq_copy(0, h, offset).wait_recv()

        @pl.when(is_given(mine, h))
        def _():
            q_copy(h, 0).wait_send()
            dq_copy(0, h, 0).wait_recv()

        @pl.when(jnp.logical_not(is_given(mine, h)))
        def _():
            dq_own(h).wait()

        @pl.when(h < taken)
        def _():
            for u in range(half):
                dq_extra(h, u).wait_send()
    for offset in range(1, spots):
        dl_copy(0, offset).wait_send()

    @pl.when(gives_now)
    def _():
        for offset in range(spots):
            dl_copy(1, offset).wait_send()

    dkv_own.wait()
    for other in range(layers):
        away = other != layer

        @pl.when(top_layer(other, layers) >= layer)
        def _():
            for offset in range(1, spots):
                kv_copy(other, offset).wait_send()
                dkv_arrival(other, offset).wait_recv()

            @pl.when(away)
            def _():
                kv_copy(other, 0).wait_send()
                dkv_arrival(other, 0).wait_recv()

        @pl.when(other <= top)
        def _():
            for offset in range(1, spots):
                dkv_copy(other, offset).wait_send()

            @pl.when(away)
            def _():
                dkv_copy(other, 0).wait_send()


def vmem(count):
    return [pl.BlockSpec(memory_space=pltpu.VMEM)] * count


def per_device(queries, key_head_matrix, value_head_matrix, attn_output, out_grad):
    seq_count = lax.axis_size("seq")
    tokens = queries.shape[1]
    group = key_head_matrix.shape[2] // (HEAD_WIDTH * seq_count)
    layers = lax.axis_size("span") // group
    spots = group * seq_count
    heads = QUERY_PER_KEY
    half = spots // 2
    pair = 2 * HEAD_WIDTH
    rows = spots * tokens

    def by_spot(source, count):
        split = source.reshape(tokens, seq_count, group, count, HEAD_WIDTH)
        return jnp.transpose(split, (2, 1, 3, 0, 4)).reshape(spots, count, tokens, HEAD_WIDTH)

    qg = jnp.concatenate([by_spot(queries[0], heads), by_spot(out_grad[0], heads)], axis=3)
    kv = jnp.concatenate([by_spot(key_head_matrix[0], 1), by_spot(value_head_matrix[0], 1)], axis=3)[:, 0]
    product = out_grad[0].astype(jnp.float32) * attn_output[0].astype(jnp.float32)
    delta = jnp.sum(product.reshape(tokens, seq_count, group, heads, HEAD_WIDTH), axis=4)
    delta = jnp.transpose(delta, (2, 1, 3, 0)).reshape(spots, heads, tokens)
    delta = jnp.pad(delta, ((0, 0), (0, 8 - heads), (0, 0)))

    tk = math.gcd(rows, 512)
    tq = half * tokens
    while layers * rows * tq * 4 > SCORE_BYTES or tk % tq:
        tq //= 2
    dma = pltpu.SemaphoreType.DMA
    dq_all, dkv_all = pl.pallas_call(
        functools.partial(kernel, group, tq, tk),
        out_shape=(
            jax.ShapeDtypeStruct((spots, heads, HEAD_WIDTH, tokens), jnp.bfloat16),
            jax.ShapeDtypeStruct((layers, spots, tokens, pair), jnp.bfloat16),
        ),
        in_specs=vmem(3),
        out_specs=tuple(vmem(2)),
        scratch_shapes=[
            pltpu.VMEM((3 * heads, half, tokens, pair), jnp.bfloat16),
            pltpu.VMEM((layers, spots, tokens, pair), jnp.bfloat16),
            pltpu.VMEM((2, spots, 8, tokens), jnp.float32),
            pltpu.VMEM((layers * rows, tq), jnp.float32),
            pltpu.VMEM((1, tq), jnp.float32),
            pltpu.VMEM((HEAD_WIDTH, tq), jnp.float32),
            pltpu.VMEM((layers * rows, pair), jnp.float32),
            pltpu.VMEM((3 * heads, half, HEAD_WIDTH, tokens), jnp.bfloat16),
            pltpu.VMEM((layers, spots, tokens, pair), jnp.bfloat16),
            dma((heads, spots)),
            dma((2, heads, spots)),
            dma((layers, spots)),
            dma((layers, spots)),
            dma((2, spots)),
            dma((2, spots)),
            dma((heads, spots)),
            dma((heads, spots)),
            dma((heads, half)),
            dma((layers, spots)),
            dma((layers, spots)),
            dma((heads,)),
            dma((heads,)),
            dma((3,)),
        ],
        compiler_params=pltpu.CompilerParams(has_side_effects=True, vmem_limit_bytes=60 * 2**20),
        name="attention_grads",
    )(qg, kv, delta)

    dq = dq_all.reshape(group, seq_count, heads * HEAD_WIDTH, tokens)
    dq = jnp.transpose(dq, (3, 1, 0, 2)).reshape(1, tokens, -1)

    def by_token(source):
        split = source.reshape(group, seq_count, tokens, source.shape[-1])
        return jnp.transpose(split, (2, 1, 0, 3)).reshape(1, tokens, -1)

    layer = lax.axis_index("span") // group
    senders = lax.broadcasted_iota(jnp.int32, (layers, 1, 1, 1), 0)
    came = top_layer(senders, layers) >= layer
    kv_sum = jnp.sum(jnp.where(came, dkv_all.astype(jnp.float32), 0.0), axis=0).astype(jnp.bfloat16)
    return dq, by_token(kv_sum[..., :HEAD_WIDTH]), by_token(kv_sum[..., HEAD_WIDTH:])


def solution(mesh):
    spec = P("span", "seq", None)
    return jax.shard_map(
        per_device, mesh=mesh, in_specs=(spec,) * 5, out_specs=(spec,) * 3, check_vma=False
    )
```

```python
import functools
import math

import jax
import jax.numpy as jnp
from jax import lax
from jax.experimental import pallas as pl
from jax.experimental.pallas import tpu as pltpu
from jax.sharding import PartitionSpec as P

HEAD_WIDTH = 64
QUERY_PER_KEY = 3
NEG_LARGE = -1e30
MESH = pl.DeviceIdType.MESH
LOG2E = math.log2(math.e)
SCORE_BYTES = 34 * 2**20


def place(group):
    seq_count = lax.axis_size("seq")
    span = lax.axis_index("span")
    layers = lax.axis_size("span") // group
    mine = lax.rem(span, group) * seq_count + lax.axis_index("seq")
    return span // group, mine, layers, group * seq_count


def device_of(layer, spot, group):
    seq_count = lax.axis_size("seq")
    return {"seq": lax.rem(spot, seq_count), "span": layer * group + spot // seq_count}


def given_heads(layer, layers):
    surplus = QUERY_PER_KEY * 2 * (2 * layer + 1 - layers)
    count = (jnp.maximum(surplus, 0) + layer + 1) // (2 * layer + 2)
    return jnp.where(surplus > 0, jnp.minimum(count, QUERY_PER_KEY), 0)


def score_blocks(layers, rows, block):
    most = 0
    per = rows // block
    for layer in range(layers):
        mirror = layers - 1 - layer
        counts = []
        for one in (layer, mirror):
            surplus = QUERY_PER_KEY * 2 * (2 * one + 1 - layers)
            count = min((max(surplus, 0) + one + 1) // (2 * one + 2), QUERY_PER_KEY)
            counts.append(count if surplus > 0 else 0)
        own = QUERY_PER_KEY * (layer * per + per // 2) + (QUERY_PER_KEY - counts[0]) * (layer + 1) * per
        most = max(most, own + counts[1] * (mirror + 1) * per)
    return most


def top_layer(layer, layers):
    mirror = layers - 1 - layer
    return jnp.where(given_heads(mirror, layers) > 0, mirror, layer)


def dot(a, b, contract):
    return lax.dot_general(a, b, ((contract[:1], contract[1:]), ((), ())), preferred_element_type=jnp.float32)


def kernel(group, tq, tk, resident, qg_ref, kv_ref, dl_ref, dq_out, dkv_out,
           qg_in, kv_in, dl_in, s_ref, dl_row, q_pad, g_pad, m_ref, l_ref, dqt_ref, acc_ref, dq_ref, dkv_ref,
           q_send, q_recv, kv_send, kv_recv, dl_send, dl_recv,
           dq_send, dq_recv, ex_send, dkv_send, dkv_recv, q_local, dq_local, local_sem):
    layer, mine, layers, spots = place(group)
    heads = QUERY_PER_KEY
    half = spots // 2
    tokens = qg_ref.shape[2]
    rows = spots * tokens
    mirror = layers - 1 - layer
    given = given_heads(layer, layers)
    taken = given_heads(mirror, layers)
    top = top_layer(layer, layers)
    scaling = 1.0 / math.sqrt(HEAD_WIDTH)
    factor = scaling * LOG2E

    def spot_at(offset):
        return lax.rem(mine + offset, spots)

    def spot_from(offset):
        return lax.rem(mine + spots - offset, spots)

    def remote(source, target, send, recv, to_layer, spot):
        return pltpu.make_async_remote_copy(
            src_ref=source, dst_ref=target, send_sem=send, recv_sem=recv,
            device_id=device_of(to_layer, spot, group), device_id_type=MESH)

    def is_given(spot, h):
        return jnp.logical_and(spot >= half, h >= heads - given)

    def q_copy(h, offset):
        away = is_given(mine, h)
        slot = jnp.where(away, heads + h + given, (mine // half) * heads + h)
        spot = spot_at(offset)
        return remote(qg_ref.at[spot, h], qg_in.at[slot, lax.rem(mine, half)],
                      q_send.at[h, offset], q_recv.at[jnp.where(away, 1, 0), h, offset],
                      jnp.where(away, mirror, layer), spot)

    def q_arrival(kind, h, offset):
        return remote(qg_ref.at[0, h], qg_in.at[0, 0], q_send.at[h, offset], q_recv.at[kind, h, offset], mirror, mine)

    def q_own(h):
        return pltpu.make_async_copy(
            qg_ref.at[mine, h], qg_in.at[(mine // half) * heads + h, lax.rem(mine, half)], q_local.at[h])

    def dl_copy(kind, offset):
        spot = spot_at(offset)
        return remote(dl_ref.at[spot], dl_in.at[kind, mine], dl_send.at[kind, offset], dl_recv.at[kind, offset],
                      layer if kind == 0 else mirror, spot)

    def kv_copy(to_layer, offset):
        spot = spot_at(offset)
        return remote(kv_ref.at[spot], kv_in.at[layer, mine], kv_send.at[to_layer, offset],
                      kv_recv.at[layer, offset], to_layer, spot)

    def kv_arrival(from_layer, offset):
        return remote(kv_ref.at[0], kv_in.at[0, 0], kv_send.at[0, offset], kv_recv.at[from_layer, offset],
                      layer, mine)

    def dq_copy(slot_base, h, offset):
        spot = spot_at(offset)
        return remote(dq_ref.at[(spot // half) * heads + h, lax.rem(spot, half)], dq_out.at[mine, h],
                      dq_send.at[h, offset], dq_recv.at[h, offset], layer, spot)

    def dq_own(h):
        return pltpu.make_async_copy(
            dq_ref.at[(mine // half) * heads + h, lax.rem(mine, half)], dq_out.at[mine, h], dq_local.at[h])

    def dq_extra(k, u):
        spot = half + u
        h = heads - taken + k
        return remote(dq_ref.at[2 * heads + k, u], dq_out.at[mine, h], ex_send.at[k, u],
                      dq_recv.at[h, lax.rem(spot + spots - mine, spots)], mirror, spot)

    def dkv_copy(to_layer, offset):
        spot = spot_at(offset)
        return remote(dkv_ref.at[to_layer, spot], dkv_out.at[layer, mine], dkv_send.at[to_layer, offset],
                      dkv_recv.at[layer, offset], to_layer, spot)

    def dkv_arrival(from_layer, offset):
        return remote(dkv_ref.at[0, 0], dkv_out.at[0, 0], dkv_send.at[0, offset],
                      dkv_recv.at[from_layer, offset], layer, mine)

    kv_own = pltpu.make_async_copy(kv_ref.at[mine], kv_in.at[layer, mine], local_sem.at[0])
    dl_own = pltpu.make_async_copy(dl_ref.at[mine], dl_in.at[0, mine], local_sem.at[1])
    dkv_own = pltpu.make_async_copy(dkv_ref.at[layer, mine], dkv_out.at[layer, mine], local_sem.at[2])
    gives_now = jnp.logical_and(mine >= half, given > 0)

    for h in range(heads):
        @pl.when(is_given(mine, h))
        def _():
            for offset in range(spots):
                q_copy(h, offset).start()

    @pl.when(gives_now)
    def _():
        for offset in range(spots):
            dl_copy(1, offset).start()

    for offset in range(spots):
        for step in range(layers - 1, 0, -1):
            other = lax.rem(layer + step, layers)

            @pl.when(top_layer(other, layers) >= layer)
            def _():
                kv_copy(other, offset).start()

        if offset:
            kv_copy(layer, offset).start()
            dl_copy(0, offset).start()
        else:
            kv_own.start()
            dl_own.start()
        for h in range(heads):
            @pl.when(jnp.logical_not(is_given(mine, h)))
            def _():
                if offset:
                    q_copy(h, offset).start()
                else:
                    q_own(h).start()

    blocks_here = rows // tk

    def clear(j, _):
        acc_ref[pl.ds(pl.multiple_of(j * tk, tk), tk), :] = jnp.zeros((tk, 2 * HEAD_WIDTH), jnp.float32)
        return 0

    lax.fori_loop(0, (top + 1) * blocks_here, clear, 0)

    kv_own.wait()
    dl_own.wait()
    for offset in range(1, spots):
        dl_copy(0, offset).wait_recv()
        kv_arrival(layer, offset).wait_recv()
    for h in range(heads):
        for offset in range(1, spots):
            @pl.when(jnp.logical_not(is_given(spot_from(offset), h)))
            def _():
                q_arrival(0, h, offset).wait_recv()

        @pl.when(jnp.logical_not(is_given(mine, h)))
        def _():
            q_own(h).wait()

    subs = half * tokens // tq
    pieces = tq // tokens
    lane = lax.broadcasted_iota(jnp.int32, (1, 2 * HEAD_WIDTH), 1)
    own_jobs = (2 * heads - given) * subs
    jobs = (2 * heads - given + taken) * subs

    def job_place(i):
        slot = i // subs
        sub = lax.rem(i, subs)
        extra = slot >= 2 * heads
        q_layer = jnp.where(extra, mirror, layer)
        q_first = q_layer * rows + jnp.where(slot >= heads, half * tokens, 0) + sub * tq
        low_blocks = layer * blocks_here + blocks_here // 2
        high_blocks = (layer + 1) * blocks_here
        base = jnp.where(slot < heads, slot * low_blocks, heads * low_blocks + (slot - heads) * high_blocks)
        base = jnp.where(extra, heads * (low_blocks + high_blocks) + (slot - 2 * heads) * (mirror + 1) * blocks_here,
                         base)
        return slot, sub, extra, q_first, q_first // tk, base

    def prepare(i, _):
        slot, sub, extra, _, _, _ = job_place(i)
        head = jnp.where(extra, slot - heads - taken, lax.rem(slot, heads))
        both = qg_in[slot, pl.ds(sub * pieces, pieces)].reshape(tq, 2 * HEAD_WIDTH)
        q_pad[i] = jnp.where(lane < HEAD_WIDTH, both, jnp.zeros_like(both))
        g_pad[i] = jnp.where(lane < HEAD_WIDTH, jnp.zeros_like(both), both)
        for piece in range(pieces):
            spot = jnp.where(slot >= heads, half, 0) + sub * pieces + piece
            dl_row[i, :, piece * tokens:(piece + 1) * tokens] = (
                dl_in[jnp.where(extra, 1, 0), spot, pl.ds(head, 1), :])
        dqt_ref[i] = jnp.zeros((HEAD_WIDTH, tq), jnp.float32)
        m_ref[i] = jnp.full((1, tq), NEG_LARGE, jnp.float32)
        l_ref[i] = jnp.zeros((1, tq), jnp.float32)
        return 0

    def kv_block(j):
        per = tk // tokens
        at = kv_in[j // blocks_here, pl.ds(lax.rem(j, blocks_here) * per, per)]
        return at.reshape(tk, 2 * HEAD_WIDTH)

    def hide(s, j, q_first):
        k_pos = j * tk + lax.broadcasted_iota(jnp.int32, (tk, tq), 0)
        q_pos = q_first + lax.broadcasted_iota(jnp.int32, (tk, tq), 1)
        return jnp.where(k_pos <= q_pos, s, NEG_LARGE)

    def layer_stats(l, low, high):
        def one_job(i, _):
            _, _, _, q_first, last, base = job_place(i)

            def block(j, masked):
                s = dot(kv_block(j), q_pad[i], (1, 1))
                if masked:
                    s = hide(s, j, q_first)
                if resident:
                    s_ref[base + j] = s
                m_old = m_ref[i]
                m_new = jnp.maximum(m_old, jnp.max(s, axis=0, keepdims=True))
                e = jnp.exp2((s - m_new) * factor)
                l_ref[i] = l_ref[i] * jnp.exp2((m_old - m_new) * factor) + jnp.sum(e, axis=0, keepdims=True)
                m_ref[i] = m_new
                return 0

            end = (l + 1) * blocks_here
            lax.fori_loop(l * blocks_here, jnp.minimum(end, last), lambda j, _: block(j, False), 0)

            @pl.when(last < end)
            def _():
                @pl.when(last >= l * blocks_here)
                def _():
                    block(last, True)
            return 0

        lax.fori_loop(low, high, one_job, 0)

    def wait_layer(l):
        for offset in range(spots):
            kv_arrival(l, offset).wait_recv()

    lax.fori_loop(0, own_jobs, prepare, 0)

    def own_stats(t, _):
        l = layer - t

        @pl.when(t > 0)
        def _():
            wait_layer(l)

        layer_stats(l, 0, own_jobs)
        return 0

    lax.fori_loop(0, layer + 1, own_stats, 0)

    @pl.when(taken > 0)
    def _():
        for offset in range(spots):
            @pl.when(spot_from(offset) >= half)
            def _():
                dl_copy(1, offset).wait_recv()
                for h in range(heads):
                    @pl.when(h >= heads - taken)
                    def _():
                        q_arrival(1, h, offset).wait_recv()

        lax.fori_loop(own_jobs, jobs, prepare, 0)

        def extra_stats(l, _):
            @pl.when(l > layer)
            def _():
                wait_layer(l)

            layer_stats(l, own_jobs, jobs)
            return 0

        lax.fori_loop(0, top + 1, extra_stats, 0)

    def norms(i, _):
        m_ref[i] = m_ref[i] * factor + jnp.log2(l_ref[i])
        return 0

    lax.fori_loop(0, jobs, norms, 0)

    def layer_grads(t, _):
        above = top - layer
        l = jnp.where(t < above, top - t, t - above)

        def one_job(i, _):
            slot, sub, extra, q_first, last, base = job_place(i)

            def grads(j, _):
                at = pl.ds(pl.multiple_of(j * tk, tk), tk)
                kv = kv_block(j)
                if resident:
                    s = s_ref[base + j]
                else:
                    s = hide(dot(kv, q_pad[i], (1, 1)), j, q_first)
                p = jnp.exp2(s * factor - m_ref[i])
                dp = dot(kv, g_pad[i], (1, 1))
                ds = (p * (dp - dl_row[i])).astype(jnp.bfloat16)
                acc_ref[at, :] += dot(ds, q_pad[i], (1, 0)) + dot(p.astype(jnp.bfloat16), g_pad[i], (1, 0))
                dqt_ref[i] += dot(kv[:, :HEAD_WIDTH].T, ds, (1, 0))
                return 0

            lax.fori_loop(l * blocks_here, jnp.minimum((l + 1) * blocks_here, last + 1), grads, 0)

            @pl.when(t == top)
            def _():
                for piece in range(pieces):
                    part = dqt_ref[i, :, piece * tokens:(piece + 1) * tokens] * scaling
                    dq_ref[slot, sub * pieces + piece] = part.astype(jnp.bfloat16)

                @pl.when(jnp.logical_and(sub == subs - 1, extra))
                def _():
                    for u in range(half):
                        dq_extra(slot - 2 * heads, u).start()

                @pl.when(jnp.logical_and(sub == subs - 1, jnp.logical_not(extra)))
                def _():
                    for offset in range(spots):
                        @pl.when(spot_at(offset) // half == slot // heads)
                        def _():
                            if offset:
                                dq_copy(0, lax.rem(slot, heads), offset).start()
                            else:
                                dq_own(lax.rem(slot, heads)).start()
            return 0

        lax.fori_loop(0, jobs, one_job, 0)

        def finish(spot, _):
            at = pl.ds(pl.multiple_of(l * rows + spot * tokens, tokens), tokens)
            part = acc_ref[at, :] * jnp.where(lane < HEAD_WIDTH, scaling, 1.0)
            dkv_ref[l, spot] = part.astype(jnp.bfloat16)
            return 0

        lax.fori_loop(0, spots, finish, 0)
        for offset in range(1, spots):
            dkv_copy(l, offset).start()

        @pl.when(l == layer)
        def _():
            dkv_own.start()

        @pl.when(l != layer)
        def _():
            dkv_copy(l, 0).start()
        return 0

    lax.fori_loop(0, top + 1, layer_grads, 0)

    for h in range(heads):
        for offset in range(1, spots):
            q_copy(h, offset).wait_send()

            @pl.when(jnp.logical_not(is_given(spot_at(offset), h)))
            def _():
                dq_copy(0, h, offset).wait_send()
            dq_copy(0, h, offset).wait_recv()

        @pl.when(is_given(mine, h))
        def _():
            q_copy(h, 0).wait_send()
            dq_copy(0, h, 0).wait_recv()

        @pl.when(jnp.logical_not(is_given(mine, h)))
        def _():
            dq_own(h).wait()

        @pl.when(h < taken)
        def _():
            for u in range(half):
                dq_extra(h, u).wait_send()
    for offset in range(1, spots):
        dl_copy(0, offset).wait_send()

    @pl.when(gives_now)
    def _():
        for offset in range(spots):
            dl_copy(1, offset).wait_send()

    dkv_own.wait()
    for other in range(layers):
        away = other != layer

        @pl.when(top_layer(other, layers) >= layer)
        def _():
            for offset in range(1, spots):
                kv_copy(other, offset).wait_send()
                dkv_arrival(other, offset).wait_recv()

            @pl.when(away)
            def _():
                kv_copy(other, 0).wait_send()
                dkv_arrival(other, 0).wait_recv()

        @pl.when(other <= top)
        def _():
            for offset in range(1, spots):
                dkv_copy(other, offset).wait_send()

            @pl.when(away)
            def _():
                dkv_copy(other, 0).wait_send()


def vmem(count):
    return [pl.BlockSpec(memory_space=pltpu.VMEM)] * count


def per_device(queries, key_head_matrix, value_head_matrix, attn_output, out_grad):
    seq_count = lax.axis_size("seq")
    tokens = queries.shape[1]
    group = key_head_matrix.shape[2] // (HEAD_WIDTH * seq_count)
    layers = lax.axis_size("span") // group
    spots = group * seq_count
    heads = QUERY_PER_KEY
    half = spots // 2
    pair = 2 * HEAD_WIDTH
    rows = spots * tokens

    def by_spot(source, count):
        split = source.reshape(tokens, seq_count, group, count, HEAD_WIDTH)
        return jnp.transpose(split, (2, 1, 3, 0, 4)).reshape(spots, count, tokens, HEAD_WIDTH)

    qg = jnp.concatenate([by_spot(queries[0], heads), by_spot(out_grad[0], heads)], axis=3)
    kv = jnp.concatenate([by_spot(key_head_matrix[0], 1), by_spot(value_head_matrix[0], 1)], axis=3)[:, 0]
    product = out_grad[0].astype(jnp.float32) * attn_output[0].astype(jnp.float32)
    delta = jnp.sum(product.reshape(tokens, seq_count, group, heads, HEAD_WIDTH), axis=4)
    delta = jnp.transpose(delta, (2, 1, 3, 0)).reshape(spots, heads, tokens)
    delta = jnp.pad(delta, ((0, 0), (0, 8 - heads), (0, 0)))

    tk = math.gcd(rows, 512)
    tq = half * tokens
    while tq > tk or tk % tq:
        tq //= 2
    count = score_blocks(layers, rows, tk)
    resident = tq == tk == half * tokens and count * tk * tq * 4 <= SCORE_BYTES
    slots = 3 * heads
    all_jobs = slots * half * tokens // tq
    dma = pltpu.SemaphoreType.DMA
    dq_all, dkv_all = pl.pallas_call(
        functools.partial(kernel, group, tq, tk, resident),
        out_shape=(
            jax.ShapeDtypeStruct((spots, heads, HEAD_WIDTH, tokens), jnp.bfloat16),
            jax.ShapeDtypeStruct((layers, spots, tokens, pair), jnp.bfloat16),
        ),
        in_specs=vmem(3),
        out_specs=tuple(vmem(2)),
        scratch_shapes=[
            pltpu.VMEM((3 * heads, half, tokens, pair), jnp.bfloat16),
            pltpu.VMEM((layers, spots, tokens, pair), jnp.bfloat16),
            pltpu.VMEM((2, spots, 8, tokens), jnp.float32),
            pltpu.VMEM((count, tk, tq) if resident else (1, 8, tq), jnp.float32),
            pltpu.VMEM((all_jobs, 1, tq), jnp.float32),
            pltpu.VMEM((all_jobs, tq, pair), jnp.bfloat16),
            pltpu.VMEM((all_jobs, tq, pair), jnp.bfloat16),
            pltpu.VMEM((all_jobs, 1, tq), jnp.float32),
            pltpu.VMEM((all_jobs, 1, tq), jnp.float32),
            pltpu.VMEM((all_jobs, HEAD_WIDTH, tq), jnp.float32),
            pltpu.VMEM((layers * rows, pair), jnp.float32),
            pltpu.VMEM((3 * heads, half, HEAD_WIDTH, tokens), jnp.bfloat16),
            pltpu.VMEM((layers, spots, tokens, pair), jnp.bfloat16),
            dma((heads, spots)),
            dma((2, heads, spots)),
            dma((layers, spots)),
            dma((layers, spots)),
            dma((2, spots)),
            dma((2, spots)),
            dma((heads, spots)),
            dma((heads, spots)),
            dma((heads, half)),
            dma((layers, spots)),
            dma((layers, spots)),
            dma((heads,)),
            dma((heads,)),
            dma((3,)),
        ],
        compiler_params=pltpu.CompilerParams(has_side_effects=True, vmem_limit_bytes=60 * 2**20),
        name="attention_grads",
    )(qg, kv, delta)

    dq = dq_all.reshape(group, seq_count, heads * HEAD_WIDTH, tokens)
    dq = jnp.transpose(dq, (3, 1, 0, 2)).reshape(1, tokens, -1)

    def by_token(source):
        split = source.reshape(group, seq_count, tokens, source.shape[-1])
        return jnp.transpose(split, (2, 1, 0, 3)).reshape(1, tokens, -1)

    layer = lax.axis_index("span") // group
    senders = lax.broadcasted_iota(jnp.int32, (layers, 1, 1, 1), 0)
    came = top_layer(senders, layers) >= layer
    kv_sum = jnp.sum(jnp.where(came, dkv_all.astype(jnp.float32), 0.0), axis=0).astype(jnp.bfloat16)
    return dq, by_token(kv_sum[..., :HEAD_WIDTH]), by_token(kv_sum[..., HEAD_WIDTH:])


def solution(mesh):
    spec = P("span", "seq", None)
    return jax.shard_map(
        per_device, mesh=mesh, in_specs=(spec,) * 5, out_specs=(spec,) * 3, check_vma=False
    )
```
